32 devices in a mesh: tp: 4 (over z), dp: 8 (over y, x, core).
Axes of the slice: x: 2, y: 2, z: 4, core: 2. Of those that a mesh axis runs over, the one named last changes fastest.
Arguments:
- feats: bfloat16 [4096, 49, 768], P('dp')
- ln_gamma: float32 [768], replicated
- ln_beta: float32 [768], replicated
- w_head: bfloat16 [768, 22528], P(None, 'tp')
- b_head: float32 [22528], P('tp')
- labels: int32 [4096], P('dp')
Outputs:
- output 1: float32 [], replicated
- output 2: bfloat16 [4096, 49, 768], P('dp')
- output 3: float32 [768, 22528], P(None, 'tp')
- output 4: float32 [22528], P('tp')
- output 5: float32 [768], replicated
- output 6: float32 [768], replicated
All inputs are finite; a program needn't handle non-finite values.
Results may differ from the reference program's by a relative error of at most 0.001.
Values sent between devices are 32-bit elements.
A program may use at most 1 GiB of HBM per device.

```python
import jax
import jax.numpy as jnp
from jax import lax

GLOBAL_BATCH = 4096
TOKENS = 49
WIDTH = 768
CLASSES = 21841
PADDED_CLASSES = 22528
ROW_BLOCK = min(GLOBAL_BATCH, 64)
LN_EPS = 1e-5
SMOOTH = 0.1


def setup_inputs(seed: int = 0) -> dict:
    sub_keys = jax.random.split(jax.random.key(seed), 7)
    image_shared = jax.random.normal(sub_keys[0], (GLOBAL_BATCH, 1, WIDTH), jnp.float32)
    token_noise = jax.random.normal(sub_keys[1], (GLOBAL_BATCH, TOKENS, WIDTH), jnp.float32)
    feats = (image_shared + 0.5 * token_noise).astype(jnp.bfloat16)
    ln_gamma = 1.0 + 0.3 * jax.random.normal(sub_keys[2], (WIDTH,), jnp.float32)
    ln_beta = 0.3 * jax.random.normal(sub_keys[3], (WIDTH,), jnp.float32)
    w_scale = 3.0 * WIDTH ** -0.5
    w_head = (w_scale * jax.random.normal(sub_keys[4], (WIDTH, PADDED_CLASSES), jnp.float32)).astype(jnp.bfloat16)
    b_head = 0.5 * jax.random.normal(sub_keys[5], (PADDED_CLASSES,), jnp.float32)
    labels = jax.random.randint(sub_keys[6], (GLOBAL_BATCH,), 0, CLASSES, dtype=jnp.int32)
    labels = labels.at[0].set(0).at[GLOBAL_BATCH - 1].set(CLASSES - 1)
    return {"feats": feats, "ln_gamma": ln_gamma, "ln_beta": ln_beta, "w_head": w_head, "b_head": b_head, "labels": labels}


def norm_pool(feats, ln_gamma, ln_beta):
    x_val = feats.astype(jnp.float32)
    mean_x = jnp.mean(x_val, axis=-1, keepdims=True)
    centered = x_val - mean_x
    var_x = jnp.mean(centered * centered, axis=-1, keepdims=True)
    inv_std = lax.rsqrt(var_x + LN_EPS)
    x_hat = centered * inv_std
    x_hat_mean = jnp.mean(x_hat, axis=1)
    pooled16 = (x_hat_mean * ln_gamma + ln_beta).astype(jnp.bfloat16)
    return x_hat, inv_std, x_hat_mean, pooled16


def norm_backward(grad_pool, x_hat, inv_std, x_hat_mean, ln_gamma):
    grad_gamma = jnp.sum(grad_pool * x_hat_mean, axis=0)
    grad_beta = jnp.sum(grad_pool, axis=0)
    upstream = grad_pool * ln_gamma / TOKENS
    up_mean = jnp.mean(upstream, axis=-1)
    proj_term = jnp.mean(x_hat * upstream[:, None, :], axis=-1, keepdims=True)
    grad_x = inv_std * (upstream[:, None, :] - up_mean[:, None, None] - x_hat * proj_term)
    return grad_x.astype(jnp.bfloat16), grad_gamma, grad_beta


def head_rows(feat_rows, label_rows, ln_gamma, ln_beta, w_head, b_head):
    x_hat, inv_std, x_hat_mean, pooled16 = norm_pool(feat_rows, ln_gamma, ln_beta)
    col_ids = jnp.arange(PADDED_CLASSES)
    valid_mask = col_ids < CLASSES
    logits = jnp.dot(pooled16, w_head, preferred_element_type=jnp.float32) + b_head
    logits = jnp.where(valid_mask, logits, -1e30)
    row_max = jnp.max(logits, axis=-1, keepdims=True)
    log_norm = row_max + jnp.log(jnp.sum(jnp.exp(logits - row_max), axis=-1, keepdims=True))
    onehot = col_ids == label_rows[:, None]
    target = jnp.sum(jnp.where(onehot, logits, 0.0), axis=-1)
    valid_sum = jnp.sum(jnp.where(valid_mask, logits, 0.0), axis=-1)
    loss_rows = log_norm[:, 0] - (1.0 - SMOOTH) * target - (SMOOTH / CLASSES) * valid_sum
    soft_probs = jnp.exp(logits - log_norm)
    dlogit = (soft_probs - (1.0 - SMOOTH) * onehot - (SMOOTH / CLASSES) * valid_mask) / GLOBAL_BATCH
    dlogit16 = dlogit.astype(jnp.bfloat16)
    grad_w = jnp.dot(pooled16.T, dlogit16, preferred_element_type=jnp.float32)
    grad_b = jnp.sum(dlogit, axis=0)
    grad_pool = jnp.dot(dlogit16, w_head.T, preferred_element_type=jnp.float32)
    grad_x, grad_gamma, grad_beta = norm_backward(grad_pool, x_hat, inv_std, x_hat_mean, ln_gamma)
    return jnp.sum(loss_rows), grad_x, grad_w, grad_b, grad_gamma, grad_beta


def reference(feats, ln_gamma, ln_beta, w_head, b_head, labels):
    block_count = GLOBAL_BATCH // ROW_BLOCK
    feat_blocks = feats.reshape(block_count, ROW_BLOCK, TOKENS, WIDTH)
    label_blocks = labels.reshape(block_count, ROW_BLOCK)
    init_carry = (jnp.zeros((), jnp.float32), jnp.zeros((WIDTH, PADDED_CLASSES), jnp.float32), jnp.zeros((PADDED_CLASSES,), jnp.float32), jnp.zeros((WIDTH,), jnp.float32), jnp.zeros((WIDTH,), jnp.float32))

    def scan_step(acc_carry, block_in):
        loss_sum, grad_x, grad_w, grad_b, grad_gamma, grad_beta = head_rows(block_in[0], block_in[1], ln_gamma, ln_beta, w_head, b_head)
        new_carry = (acc_carry[0] + loss_sum, acc_carry[1] + grad_w, acc_carry[2] + grad_b, acc_carry[3] + grad_gamma, acc_carry[4] + grad_beta)
        return new_carry, grad_x

    final_carry, grad_blocks = lax.scan(scan_step, init_carry, (feat_blocks, label_blocks))
    grad_feats = grad_blocks.reshape(GLOBAL_BATCH, TOKENS, WIDTH)
    return (final_carry[0] / GLOBAL_BATCH, grad_feats, final_carry[1], final_carry[2], final_carry[3], final_carry[4])
```

```python
import functools
import jax
import jax.numpy as jnp
from jax import lax
from jax.experimental import pallas as pl
from jax.experimental.pallas import tpu as pltpu
from jax.sharding import PartitionSpec as P

VALID_CLASSES = 21841
LN_EPS = 1e-5
SMOOTH = 0.1
BATCH = 4096
TOKENS = 49
WIDTH = 768
HALF = 2816
TILE = 256
NT = HALF // TILE
NPLAIN = 8
RB = 256
NB = BATCH // RB
ROWS = 512
SUB = 32
PROWS = WIDTH + 8
ARC = 6
VMEM_ALL = 64 * 1024 * 1024 - 65536
F32 = jnp.float32
BF16 = jnp.bfloat16


def coords():
    z = lax.axis_index("tp")
    dp = lax.axis_index("dp")
    c = lax.rem(dp, 2)
    x = lax.rem(dp // 2, 2)
    y = dp // 4
    return z, dp, y, x, c


def ln_gather_kernel(f_hbm, lab_ref, gam_ref, bet_ref, pall, xhm_ref, stat_ref,
                     fbuf, pbuf, psend, fsem, loc, sx, sy, sc, rx, ry, rc):
    z, dp, y, x, c = coords()
    dpx = dp + 2 - 4 * x
    dpy = dp + 4 - 8 * y
    dpc = dp + 1 - 2 * c
    dpd = dpx + 4 - 8 * y

    bar = pltpu.get_barrier_semaphore()
    for d in (dpx, dpy, dpc):
        pl.semaphore_signal(bar, inc=1, device_id={"dp": d}, device_id_type=pl.DeviceIdType.MESH)

    def load(i, slot):
        return pltpu.make_async_copy(f_hbm.at[:, pl.ds(pl.multiple_of(i * SUB, SUB), SUB), :], fbuf.at[slot], fsem.at[slot])

    def rcopy(src, chunk, ss, rs, dev):
        return pltpu.make_async_remote_copy(src_ref=src, dst_ref=pall.at[chunk], send_sem=ss, recv_sem=rs,
                                            device_id={"dp": dev}, device_id_type=pl.DeviceIdType.MESH)

    load(0, 0).start()
    lane = lax.broadcasted_iota(jnp.int32, (16, 128), 1)

    def sub_step(k, s, carry):
        i = k * 4 + s
        slot = lax.rem(i, 2)

        @pl.when(i + 1 < ROWS // SUB)
        def _():
            load(i + 1, 1 - slot).start()

        load(i, slot).wait()
        for rt in range(SUB // 16):
            row = pl.multiple_of(i * SUB + rt * 16, 16)

            def group(g, acc):
                st = jnp.zeros((16, 128), F32)
                for j in range(7):
                    v = fbuf[slot, g * 7 + j, rt * 16:rt * 16 + 16, :].astype(F32)
                    m = jnp.sum(v, axis=-1, keepdims=True) * (1.0 / WIDTH)
                    cv = v - m
                    inv = lax.rsqrt(jnp.sum(cv * cv, axis=-1, keepdims=True) * (1.0 / WIDTH) + LN_EPS)
                    acc = acc + cv * inv
                    st = jnp.where(lane == j, m, jnp.where(lane == 64 + j, inv, st))
                stat_ref[g, pl.ds(row, 16), :] = st
                return acc

            acc = lax.fori_loop(0, 7, group, jnp.zeros((16, WIDTH), F32))
            xh = acc * (1.0 / TOKENS)
            xhm_ref[pl.ds(row, 16), :] = xh
            pv = (xh * gam_ref[...] + bet_ref[...]).astype(BF16).astype(F32)
            pbuf[pl.ds(pl.multiple_of(s * SUB + rt * 16, 16), 16), :] = pv
        return carry

    sends = []
    locals_ = []
    for k in range(4):
        lax.fori_loop(0, 4, functools.partial(sub_step, k), 0)
        psend[k, 0:WIDTH, :] = pbuf[...].T
        psend[k, WIDTH:PROWS, :] = jnp.broadcast_to(lab_ref[k], (8, 128))
        if k == 0:
            pl.semaphore_wait(bar, 3)
        ch = dp * 4 + k
        for cp in (rcopy(psend.at[k], ch, sx.at[k], rx.at[k], dpx),
                   rcopy(psend.at[k], ch, sy.at[k], ry.at[k], dpy),
                   rcopy(psend.at[k], ch, sc.at[k], rc.at[k], dpc)):
            cp.start()
            sends.append(cp)
        lc = pltpu.make_async_copy(psend.at[k], pall.at[ch], loc.at[k])
        lc.start()
        locals_.append(lc)

    def relay(chunk, ss, rs, dev):
        cp = rcopy(pall.at[chunk], chunk, ss, rs, dev)
        cp.start()
        sends.append(cp)

    for k in range(4):
        cx = dpx * 4 + k
        rcopy(pall.at[cx], cx, sx.at[k], rx.at[k], dpx).wait_recv()
        if k < 2:
            relay(cx, sy.at[4 + k], ry.at[4 + k], dpy)
        relay(cx, sc.at[4 + k], rc.at[4 + k], dpc)
        cy = dpy * 4 + k
        rcopy(pall.at[cy], cy, sy.at[k], ry.at[k], dpy).wait_recv()
        if k >= 2:
            relay(cy, sx.at[2 + k], rx.at[2 + k], dpx)
        relay(cy, sc.at[8 + k], rc.at[8 + k], dpc)
    for k in range(4):
        cd = dpd * 4 + k
        if k < 2:
            rcopy(pall.at[cd], cd, sy.at[4 + k], ry.at[4 + k], dpy).wait_recv()
        else:
            rcopy(pall.at[cd], cd, sx.at[2 + k], rx.at[2 + k], dpx).wait_recv()
        relay(cd, sc.at[12 + k], rc.at[12 + k], dpc)
    for q, d in enumerate((dp, dpx, dpy, dpd)):
        for k in range(4):
            ch = (d + 1 - 2 * c) * 4 + k
            rcopy(pall.at[ch], ch, sc.at[q * 4 + k], rc.at[q * 4 + k], dpc).wait_recv()
    for cp in sends:
        cp.wait_send()
    for cp in locals_:
        cp.wait()


def ln_gather(f_t, lab, gam, bet):
    dma = pltpu.SemaphoreType.DMA
    vm = pl.BlockSpec(memory_space=pltpu.VMEM)
    hbm = pl.BlockSpec(memory_space=pl.ANY)
    return pl.pallas_call(
        ln_gather_kernel,
        out_shape=(jax.ShapeDtypeStruct((BATCH // 128, PROWS, 128), F32),
                   jax.ShapeDtypeStruct((ROWS, WIDTH), F32),
                   jax.ShapeDtypeStruct((7, ROWS, 128), F32)),
        in_specs=[hbm, vm, vm, vm],
        out_specs=(hbm, vm, vm),
        scratch_shapes=[pltpu.VMEM((2, TOKENS, SUB, WIDTH), BF16), pltpu.VMEM((128, WIDTH), F32),
                        pltpu.VMEM((4, PROWS, 128), F32), dma((2,)), dma((4,)),
                        dma((6,)), dma((6,)), dma((16,)), dma((6,)), dma((6,)), dma((16,))],
        compiler_params=pltpu.CompilerParams(collective_id=0, has_side_effects=True, vmem_limit_bytes=VMEM_ALL),
        name="ln_gather",
    )(f_t, lab, gam, bet)


def head_kernel(pall, wt_ref, w_hbm, b_ref, iota_ref, dpool_ref, dwo, dwr, db_ref, dbr, loss_ref,
                dlt, ering, ptb, pbuf, ylab, sbuf, dpa, d2d, ubuf, dbuf, dsend, dwt,
                psem, wsem, ss, rs, cs, cr, us, ur, ds_, dr, dls, dss, dsr, bs, br):
    z, dp, y, x, c = coords()
    dpc = dp + 1 - 2 * c
    me = z * 2 + c
    MESH = pl.DeviceIdType.MESH
    colbase = (z * 2 + c) * HALF
    colbase_f = colbase.astype(F32)
    limit_f = (VALID_CLASSES - colbase).astype(F32)

    bar = pltpu.get_barrier_semaphore()
    for j in range(7):
        p = lax.rem(me + 1 + j, 8)
        pl.semaphore_signal(bar, inc=1, device_id={"tp": p // 2, "dp": dp - c + lax.rem(p, 2)}, device_id_type=MESH)

    wcopy = pltpu.make_async_copy(w_hbm, dlt.at[0:WIDTH, 1024:1024 + HALF], wsem)
    wcopy.start()

    def chunk_of(r, h):
        q = r // 2
        qc = q // 2
        gx = lax.rem(x + lax.rem(qc, 2), 2)
        gy = lax.rem(y + qc // 2, 2)
        return (gy * 4 + gx * 2 + lax.rem(q, 2)) * 4 + lax.rem(r, 2) * 2 + h

    def ploads(r):
        slot = lax.rem(r, 2)
        return [pltpu.make_async_copy(pall.at[chunk_of(r, h)], pbuf.at[slot, h], psem.at[slot, h]) for h in range(2)]

    for cp in ploads(0):
        cp.start()
    db_ref[...] = jnp.zeros_like(db_ref)
    loss_ref[...] = jnp.zeros_like(loss_ref)
    pl.semaphore_wait(bar, 7)

    def ci():
        v = iota_ref[...]
        return jnp.concatenate([v, v], axis=1)

    def fwd_block(r):
        slot = lax.rem(r, 2)

        @pl.when(r + 1 < NB)
        def _():
            for cp in ploads(r + 1):
                cp.start()

        for cp in ploads(r):
            cp.wait()
        pb = jnp.concatenate([pbuf[slot, 0, 0:WIDTH, :], pbuf[slot, 1, 0:WIDTH, :]], axis=1).astype(BF16)
        lanes = pl.ds(pl.multiple_of(r * RB, RB), RB)
        ptb[:, lanes] = pb
        yb = jnp.concatenate([pbuf[slot, 0, WIDTH:PROWS, :], pbuf[slot, 1, WIDTH:PROWS, :]], axis=1) - colbase_f
        ylab[r] = yb
        es = lax.rem(r, 4)

        def pass1(n, masked, carry):
            mx, tg, vs = carry
            rows = pl.ds(pl.multiple_of(n * TILE, TILE), TILE)
            bb = b_ref[rows, :]
            l = jnp.dot(wt_ref[rows, :], ptb[:, lanes], preferred_element_type=F32) + jnp.concatenate([bb, bb], axis=1)
            off = lax.convert_element_type(n * TILE, F32)
            yy = jnp.broadcast_to((yb - off)[None], (TILE // 8, 8, RB)).reshape(TILE, RB)
            hot = ci() == yy
            tg = tg + jnp.where(hot, l, 0.0).reshape(TILE // 8, 8, RB).sum(axis=0)
            vs = vs + l.reshape(TILE // 8, 8, RB).sum(axis=0)
            if masked:
                l = jnp.where(ci() < limit_f - off, l, -1e30)
            ering[es, rows, :] = l
            mx = jnp.maximum(mx, l.reshape(TILE // 8, 8, RB).max(axis=0))
            return mx, tg, vs

        zero = jnp.zeros((8, RB), F32)
        carry = (jnp.full((8, RB), -3e38, F32), zero, zero)
        carry = lax.fori_loop(0, NPLAIN, lambda n, cr_: pass1(n, False, cr_), carry)
        carry = lax.fori_loop(NPLAIN, NT, lambda n, cr_: pass1(n, True, cr_), carry)
        mx, tg, vs = carry
        m = jnp.max(mx, axis=0, keepdims=True)
        mb = jnp.broadcast_to(m, (TILE, RB))

        def pass2(n, s):
            rows = pl.ds(pl.multiple_of(n * TILE, TILE), TILE)
            e = jnp.exp(ering[es, rows, :] - mb)
            ering[es, rows, :] = e
            return s + e.reshape(TILE // 8, 8, RB).sum(axis=0)

        s = lax.fori_loop(0, NT, pass2, zero)
        sbuf[r, 7, 0:1, :] = m
        sbuf[r, 7, 1:2, :] = jnp.sum(s, axis=0, keepdims=True)
        sbuf[r, 7, 2:3, :] = jnp.sum(tg, axis=0, keepdims=True)
        sbuf[r, 7, 3:4, :] = jnp.sum(vs, axis=0, keepdims=True)
        for j in range(7):
            p = lax.rem(me + 1 + j, 8)
            pltpu.make_async_remote_copy(
                src_ref=sbuf.at[r, 7], dst_ref=sbuf.at[r, 6 - j], send_sem=ss.at[r, j], recv_sem=rs.at[r, 6 - j],
                device_id={"tp": p // 2, "dp": dp - c + lax.rem(p, 2)}, device_id_type=MESH).start()

    c0 = (SMOOTH / VALID_CLASSES) / BATCH
    c1 = c0 + (1.0 - SMOOTH) / BATCH

    def dl_block(r):
        es = lax.rem(r, 4)
        for j in range(7):
            p = lax.rem(me + 1 + j, 8)
            cp = pltpu.make_async_remote_copy(
                src_ref=sbuf.at[r, 7], dst_ref=sbuf.at[r, j], send_sem=ss.at[r, j], recv_sem=rs.at[r, j],
                device_id={"tp": p // 2, "dp": dp - c + lax.rem(p, 2)}, device_id_type=MESH)
            cp.wait_recv()
            cp.wait_send()
        mown = sbuf[r, 7, 0:1, :]
        gm = mown
        for j in range(7):
            gm = jnp.maximum(gm, sbuf[r, j, 0:1, :])
        zs = jnp.zeros_like(gm)
        ts = jnp.zeros_like(gm)
        vs = jnp.zeros_like(gm)
        for j in range(8):
            zs = zs + sbuf[r, j, 1:2, :] * jnp.exp(sbuf[r, j, 0:1, :] - gm)
            ts = ts + sbuf[r, j, 2:3, :]
            vs = vs + sbuf[r, j, 3:4, :]
        loss_ref[...] += gm + jnp.log(zs) - (1.0 - SMOOTH) * ts - (SMOOTH / VALID_CLASSES) * vs
        scale = jnp.exp(mown - gm) / (zs * BATCH)
        scb = jnp.broadcast_to(scale, (TILE, RB))
        yb = ylab[r]
        lanes = pl.ds(pl.multiple_of(r * RB, RB), RB)

        def tile(n, masked):
            rows = pl.ds(pl.multiple_of(n * TILE, TILE), TILE)
            off = lax.convert_element_type(n * TILE, F32)
            yy = jnp.broadcast_to((yb - off)[None], (TILE // 8, 8, RB)).reshape(TILE, RB)
            hot = ci() == yy
            base = jnp.where(ci() < limit_f - off, c0, 0.0) if masked else c0
            d = ering[es, rows, :] * scb - jnp.where(hot, c1, base)
            db_ref[rows, :] += d[:, 0:128] + d[:, 128:256]
            dlt[rows, lanes] = d.astype(BF16)

        def plain(n, cr_):
            tile(n, False)
            return cr_

        def mask(n, cr_):
            tile(n, True)
            return cr_

        lax.fori_loop(0, NPLAIN, plain, 0)
        lax.fori_loop(NPLAIN, NT, mask, 0)

    def own_fwd(r, cr_):
        fwd_block(r)
        return cr_

    def own_dl(r, cr_):
        dl_block(r)
        return cr_

    lax.fori_loop(0, 4, own_fwd, 0)
    lax.fori_loop(0, 4, own_dl, 0)
    wcopy.wait()

    def dpool_block(i, cr_):
        lanes = pl.ds(pl.multiple_of(i * RB, RB), RB)
        dpa[i] = jnp.dot(dlt[0:WIDTH, 1024:1024 + HALF], dlt[:, lanes], preferred_element_type=F32)
        return cr_

    lax.fori_loop(0, 4, dpool_block, 0)
    d2c = pltpu.make_async_remote_copy(
        src_ref=dpa.at[pl.ds((1 - c) * 2, 2)], dst_ref=d2d, send_sem=cs, recv_sem=cr,
        device_id={"dp": dpc}, device_id_type=MESH)
    d2c.start()
    d2c.wait()
    for h in range(2):
        d2d[h] = d2d[h] + dpa[c * 2 + h]

    def own(j):
        rows = pl.ds(pl.multiple_of(j * 128, 128), 128)
        return jnp.concatenate([d2d[0, rows, :], d2d[1, rows, :]], axis=1)

    def up(j):
        return pltpu.make_async_remote_copy(src_ref=ubuf.at[j], dst_ref=ubuf.at[j], send_sem=us.at[j], recv_sem=ur.at[j],
                                            device_id={"tp": jnp.minimum(z + 1, 3)}, device_id_type=MESH)

    def down(j):
        return pltpu.make_async_remote_copy(src_ref=dsend.at[j], dst_ref=dbuf.at[j], send_sem=ds_.at[j], recv_sem=dr.at[j],
                                            device_id={"tp": jnp.maximum(z - 1, 0)}, device_id_type=MESH)

    @pl.when(z == 0)
    def _():
        for j in range(ARC):
            ubuf[j] = own(j)
            up(j).start()

    @pl.when(z == 3)
    def _():
        for j in range(ARC):
            dsend[j] = own(j)
            down(j).start()

    def tick(t):
        tu = t - 3 * z - 1

        @pl.when((z >= 1) & (tu >= 0) & (lax.rem(tu, 2) == 0) & (tu // 2 < ARC))
        def _():
            j = tu // 2
            up(j).wait_recv()
            ubuf[j] = ubuf[j] + own(j)

            @pl.when(z < 3)
            def _():
                up(j).start()

        td = t - 3 * (3 - z) - 1

        @pl.when((z <= 2) & (td >= 0) & (lax.rem(td, 2) == 0) & (td // 2 < ARC))
        def _():
            j = td // 2
            down(j).wait_recv()

            @pl.when(z > 0)
            def _():
                dsend[j] = dbuf[j] + own(j)
                down(j).start()

    def rest(r, cr_):
        fwd_block(r)

        @pl.when(r >= 6)
        def _():
            dl_block(r - 2)

        tick(r - 4)
        return cr_

    lax.fori_loop(4, NB, rest, 0)
    lax.fori_loop(NB - 2, NB, own_dl, 0)

    dbc = pltpu.make_async_remote_copy(src_ref=db_ref, dst_ref=dbr, send_sem=bs, recv_sem=br,
                                       device_id={"dp": dpc}, device_id_type=MESH)
    dbc.start()

    def dw_local(n):
        slot = lax.rem(n, 2)
        return pltpu.make_async_copy(dwt.at[slot], dwo.at[:, pl.ds(pl.multiple_of(n * TILE, TILE), TILE)], dls.at[slot])

    def dw_remote(n):
        slot = lax.rem(n, 2)
        return pltpu.make_async_remote_copy(
            src_ref=dwt.at[slot], dst_ref=dwr.at[:, pl.ds(pl.multiple_of(n * TILE, TILE), TILE)],
            send_sem=dss.at[slot], recv_sem=dsr.at[n], device_id={"dp": dpc}, device_id_type=MESH)

    def dw_step(n, cr_):
        @pl.when(n >= 2)
        def _():
            dw_local(n - 2).wait()
            dw_remote(n - 2).wait_send()

        rows = pl.ds(pl.multiple_of(n * TILE, TILE), TILE)
        dwt[lax.rem(n, 2)] = lax.dot_general(ptb[...], dlt[rows, :], (((1,), (1,)), ((), ())), preferred_element_type=F32)
        dw_local(n).start()
        dw_remote(n).start()
        tick(n + 12)
        return cr_

    lax.fori_loop(0, NT, dw_step, 0)

    for j in range(ARC):
        tot = jnp.where(z < 3, dbuf[j], 0.0) + ubuf[j]
        dpool_ref[:, j * 128:(j + 1) * 128] = tot.T

    for n in (NT - 2, NT - 1):
        dw_local(n).wait()
        dw_remote(n).wait_send()

    def dw_recv(n, cr_):
        dw_remote(n).wait_recv()
        return cr_

    lax.fori_loop(0, NT, dw_recv, 0)
    dbc.wait()

    @pl.when(z < 3)
    def _():
        for j in range(ARC):
            up(j).wait_send()

    @pl.when(z > 0)
    def _():
        for j in range(ARC):
            down(j).wait_send()


def head(pall, wt, w, bb, iota):
    dma = pltpu.SemaphoreType.DMA
    vm = pl.BlockSpec(memory_space=pltpu.VMEM)
    hbm = pl.BlockSpec(memory_space=pl.ANY)
    V = pltpu.VMEM
    return pl.pallas_call(
        head_kernel,
        out_shape=(jax.ShapeDtypeStruct((ROWS, WIDTH), F32),
                   jax.ShapeDtypeStruct((WIDTH, HALF), F32),
                   jax.ShapeDtypeStruct((WIDTH, HALF), F32),
                   jax.ShapeDtypeStruct((HALF, 128), F32),
                   jax.ShapeDtypeStruct((HALF, 128), F32),
                   jax.ShapeDtypeStruct((1, RB), F32)),
        in_specs=[hbm, vm, hbm, vm, vm],
        out_specs=(vm, hbm, hbm, vm, hbm, vm),
        scratch_shapes=[V((HALF, BATCH), BF16), V((4, HALF, RB), F32), V((WIDTH, BATCH), BF16),
                        V((2, 2, PROWS, 128), F32), V((NB, 8, RB), F32), V((NB, 8, 4, RB), F32),
                        V((4, WIDTH, RB), F32), V((2, WIDTH, RB), F32),
                        V((ARC, 128, ROWS), F32), V((ARC, 128, ROWS), F32), V((ARC, 128, ROWS), F32),
                        V((2, WIDTH, TILE), F32),
                        dma((2, 2)), dma, dma((NB, 7)), dma((NB, 7)), dma, dma,
                        dma((ARC,)), dma((ARC,)), dma((ARC,)), dma((ARC,)),
                        dma((2,)), dma((2,)), dma((NT,)), dma, dma],
        compiler_params=pltpu.CompilerParams(collective_id=1, has_side_effects=True, vmem_limit_bytes=VMEM_ALL),
        name="head",
    )(pall, wt, w, bb, iota)


def ln_bwd_kernel(f_ref, stat_ref, dp_ref, gam_ref, o_ref):
    for rt in range(SUB // 16):
        rs = slice(rt * 16, rt * 16 + 16)
        u = dp_ref[rs, :] * gam_ref[...] * (1.0 / TOKENS)
        u = u - jnp.sum(u, axis=-1, keepdims=True) * (1.0 / WIDTH)

        def group(g, cr_):
            st = stat_ref[g, rs, :]
            for j in range(7):
                m = st[:, j:j + 1]
                inv = st[:, 64 + j:65 + j]
                d = f_ref[g * 7 + j, rs, :].astype(F32) - m
                pr = jnp.sum(d * u, axis=-1, keepdims=True) * (1.0 / WIDTH)
                o_ref[g * 7 + j, rs, :] = (inv * u - (inv * inv * inv * pr) * d).astype(BF16)
            return cr_

        lax.fori_loop(0, 7, group, 0)


def ln_bwd(f_t, stat, dpool, gam):
    blk = pl.BlockSpec((TOKENS, SUB, WIDTH), lambda i: (0, i, 0))
    return pl.pallas_call(
        ln_bwd_kernel,
        grid=(ROWS // SUB,),
        out_shape=jax.ShapeDtypeStruct((TOKENS, ROWS, WIDTH), BF16),
        in_specs=[blk, pl.BlockSpec((7, SUB, 128), lambda i: (0, i, 0)),
                  pl.BlockSpec((SUB, WIDTH), lambda i: (i, 0)), pl.BlockSpec((1, WIDTH), lambda i: (0, 0))],
        out_specs=blk,
        name="ln_bwd",
    )(f_t, stat, dpool, gam)


def solution(mesh):
    def local(feats, gamma, beta, w, b, labels):
        z, dp, y, x, c = coords()
        f_t = jnp.transpose(feats, (1, 0, 2))
        lab = labels.astype(F32).reshape(4, 1, 128)
        col = (z * 2 + c) * HALF + jnp.arange(HALF)
        valid = col < VALID_CLASSES
        wh = jnp.where(valid[None, :], lax.dynamic_slice(w, (0, c * HALF), (WIDTH, HALF)), jnp.zeros((), BF16))
        bh = jnp.where(valid, lax.dynamic_slice(b, (c * HALF,), (HALF,)), 0.0)
        bb = jnp.broadcast_to(bh[:, None], (HALF, 128))
        iota = lax.broadcasted_iota(F32, (TILE, 128), 0)
        pall, xhm, stat = ln_gather(f_t, lab, gamma[None, :], beta[None, :])
        dpool, dwo, dwr, dbo, dbr, loss = head(pall, wh.T, wh, bb, iota)
        df_t = ln_bwd(f_t, stat, dpool, gamma[None, :])
        gsum = lax.psum(jnp.stack([jnp.sum(dpool * xhm, axis=0), jnp.sum(dpool, axis=0)]), "dp")
        dw = jnp.concatenate([jnp.where(c == 0, dwo, dwr), jnp.where(c == 0, dwr, dwo)], axis=1)
        dbs = jnp.sum(dbo, axis=1)
        dbrs = jnp.sum(dbr, axis=1)
        db = jnp.concatenate([jnp.where(c == 0, dbs, dbrs), jnp.where(c == 0, dbrs, dbs)])
        return jnp.sum(loss) / BATCH, jnp.transpose(df_t, (1, 0, 2)), dw, db, gsum[0], gsum[1]

    return jax.shard_map(local, mesh=mesh, in_specs=(P("dp", None, None), P(), P(), P(None, "tp"), P("tp"), P("dp")),
                         out_specs=(P(), P("dp", None, None), P(None, "tp"), P("tp"), P(), P()), check_vma=False)
```

```python
import functools
import jax
import jax.numpy as jnp
from jax import lax
from jax.experimental import pallas as pl
from jax.experimental.pallas import tpu as pltpu
from jax.sharding import PartitionSpec as P

VALID_CLASSES = 21841
LN_EPS = 1e-5
SMOOTH = 0.1
BATCH = 4096
TOKENS = 49
WIDTH = 768
HALF = 2816
TILE = 256
NT = HALF // TILE
LT = 1408
ET = 704
CLS = 2 * HALF
RB = 256
NB = BATCH // RB
ROWS = 512
SUB = 32
PROWS = WIDTH + 8
ARW = 64
ARC = WIDTH // ARW
LANE = 128
TG = 7
SIDE = 64
PEERS = 7
VMEM_ALL = 64 * 1024 * 1024 - 65536
F32 = jnp.float32
BF16 = jnp.bfloat16


def coords():
    z = lax.axis_index("tp")
    dp = lax.axis_index("dp")
    c = lax.rem(dp, 2)
    x = lax.rem(dp // 2, 2)
    y = dp // 4
    return z, dp, y, x, c


OWN = 4
MESH = pl.DeviceIdType.MESH
C0 = (SMOOTH / VALID_CLASSES) / BATCH
C1 = C0 + (1.0 - SMOOTH) / BATCH


def peer(j):
    z, dp, y, x, c = coords()
    p = lax.rem(z * 2 + c + 1 + j, PEERS + 1)
    return {"tp": p // 2, "dp": dp - c + lax.rem(p, 2)}


def block_code(first, pall, wt_ref, b_ref, loss_ref, dlt, ering, ptb, pbuf, ylab, sbuf, db_ref, iota_ref, psem, ss, rs):
    z, dp, y, x, c = coords()
    colbase = (z * 2 + c) * HALF
    colbase_f = colbase.astype(F32)
    limit_f = (VALID_CLASSES - colbase).astype(F32)
    halves = range(2)

    def chunk_of(r, h):
        q = r // 2
        qc = q // 2
        gx = lax.rem(x + lax.rem(qc, 2), 2)
        gy = lax.rem(y + qc // 2, 2)
        return (gy * 4 + gx * 2 + lax.rem(q, 2)) * 4 + lax.rem(r, 2) * 2 + h

    def ploads(r):
        slot = lax.rem(r, 2)
        return [pltpu.make_async_copy(pall.at[chunk_of(r, h)], pbuf.at[slot, h], psem.at[slot, h]) for h in halves]

    def shifted(yb, off, n):
        return jnp.broadcast_to((yb - off)[None], (n // 8, 8, RB)).reshape(n, RB)

    def ids(n):
        v = iota_ref[0:n, :]
        return jnp.concatenate([v, v], axis=1)

    def fold(v):
        return v.reshape(v.shape[0] // 8, 8, RB)

    def scopy(r, j, slot):
        i = r - first
        return pltpu.make_async_remote_copy(src_ref=sbuf.at[i, PEERS], dst_ref=sbuf.at[i, slot], send_sem=ss.at[i, j],
                                            recv_sem=rs.at[i, slot], device_id=peer(j), device_id_type=MESH)

    def fwd_block(r, stop):
        slot = lax.rem(r, 2)

        @pl.when(r + 1 < stop)
        def _():
            for cp in ploads(r + 1):
                cp.start()

        for cp in ploads(r):
            cp.wait()
        lanes = pl.ds(pl.multiple_of(r * RB, RB), RB)
        ptb[:, lanes] = jnp.concatenate([pbuf[slot, h, 0:WIDTH, :] for h in halves], axis=1).astype(BF16)
        yb = jnp.concatenate([pbuf[slot, h, WIDTH:PROWS, :] for h in halves], axis=1) - colbase_f
        ylab[r - first] = yb
        es = lax.rem(r, OWN)
        zero = jnp.zeros((8, RB), F32)
        mx, tg, vs = jnp.full((8, RB), -3e38, F32), zero, zero
        for n in range(HALF // LT):
            full = jnp.dot(wt_ref[n * LT:(n + 1) * LT, :], ptb[:, lanes], preferred_element_type=F32)
            for lo, size, masked in (((0, LT, 0),) if n == 0 else ((0, ET, 0), (ET, ET, 1))):
                row = n * LT + lo
                bb = b_ref[row:row + size, :]
                l = full[lo:lo + size] + jnp.concatenate([bb, bb], axis=1)
                tg = tg + fold(jnp.where(ids(size) == shifted(yb, float(row), size), l, 0.0)).sum(axis=0)
                if masked:
                    ok = ids(size) < limit_f - float(row)
                    vs = vs + fold(jnp.where(ok, l, 0.0)).sum(axis=0)
                    l = jnp.where(ok, l, -1e30)
                else:
                    vs = vs + fold(l).sum(axis=0)
                ering[es, row:row + size, :] = l
                mx = jnp.maximum(mx, fold(l).max(axis=0))
        m = jnp.max(mx, axis=0, keepdims=True)
        mb = jnp.broadcast_to(m, (ET, RB))

        def pass2(n, s):
            rows = pl.ds(pl.multiple_of(n * ET, ET), ET)
            e = jnp.exp(ering[es, rows, :] - mb)
            ering[es, rows, :] = e
            return s + fold(e).sum(axis=0)

        s = lax.fori_loop(0, HALF // ET, pass2, zero)
        tops = [m] + [jnp.sum(v, axis=0, keepdims=True) for v in (s, tg, vs)]
        for q, v in enumerate(tops):
            sbuf[r - first, PEERS, q:q + 1, :] = v
        for j in range(PEERS):
            scopy(r, j, PEERS - 1 - j).start()

    def dl_block(r):
        es = lax.rem(r, OWN)
        for j in range(PEERS):
            cp = scopy(r, j, j)
            cp.wait_recv()
            cp.wait_send()
        i = r - first
        mown = sbuf[i, PEERS, 0:1, :]
        gm = mown
        for j in range(PEERS):
            gm = jnp.maximum(gm, sbuf[i, j, 0:1, :])
        zs, ts, vs = (jnp.zeros_like(gm) for _ in range(3))
        for j in range(PEERS + 1):
            zs = zs + sbuf[i, j, 1:2, :] * jnp.exp(sbuf[i, j, 0:1, :] - gm)
            ts = ts + sbuf[i, j, 2:3, :]
            vs = vs + sbuf[i, j, 3:4, :]
        loss_ref[...] += gm + jnp.log(zs) - (1.0 - SMOOTH) * ts - (SMOOTH / VALID_CLASSES) * vs
        scb = jnp.broadcast_to(jnp.exp(mown - gm) / (zs * BATCH), (ET, RB))
        yb = ylab[i]
        lanes = pl.ds(pl.multiple_of(r * RB, RB), RB)

        def tile(n, masked):
            rows = pl.ds(pl.multiple_of(n * ET, ET), ET)
            off = lax.convert_element_type(n * ET, F32)
            base = jnp.where(ids(ET) < limit_f - off, C0, 0.0) if masked else C0
            d = ering[es, rows, :] * scb - jnp.where(ids(ET) == shifted(yb, off, ET), C1, base)
            db_ref[rows, :] += d[:, 0:LANE] + d[:, LANE:RB]
            dlt[rows, lanes] = d.astype(BF16)

        def plain(n, cr_):
            tile(n, 0)
            return cr_

        lax.fori_loop(0, HALF // ET - 1, plain, 0)
        tile(HALF // ET - 1, 1)

    return ploads, fwd_block, dl_block


def rep(v):
    return jnp.concatenate([v] * (WIDTH // 128), axis=1)


def ln_gather_kernel(f_hbm, prm, w_hbm, pall, xhm_ref, stat_ref, loss_ref, wt_o, bb_o, dlt_o, ptb_o, db_o, own_o,
                     fbuf, prow, psend, wbuf, mb, ib, ab, wt_ref, bb_ref, dlt, ering, ptb, pbuf, ylab, sbuf, db_ref, iota_ref,
                     dpa, d2d, fsem, wsem, loc, sx, sy, sc, rx, ry, rc, psem, ss, rs, cs, cr, osem):
    z, dp, y, x, c = coords()
    dpx = dp + 2 - 4 * x
    dpy = dp + 4 - 8 * y
    dpc = dp + 1 - 2 * c
    dpd = dpx + 4 - 8 * y

    bar = pltpu.get_barrier_semaphore()
    for d in (dpx, dpy, dpc):
        pl.semaphore_signal(bar, inc=1, device_id={"dp": d}, device_id_type=MESH)
    for j in range(PEERS):
        pl.semaphore_signal(bar, inc=1, device_id=peer(j), device_id_type=MESH)

    def load(i, slot):
        return pltpu.make_async_copy(f_hbm.at[:, pl.ds(pl.multiple_of(i * SUB, SUB), SUB), :], fbuf.at[slot], fsem.at[slot])

    def rcopy(src, chunk, ss, rs, dev):
        return pltpu.make_async_remote_copy(src_ref=src, dst_ref=pall.at[chunk], send_sem=ss, recv_sem=rs,
                                            device_id={"dp": dev}, device_id_type=pl.DeviceIdType.MESH)

    load(0, 0).start()
    half = pl.multiple_of(c * HALF, 128)
    wcopy = pltpu.make_async_copy(w_hbm.at[:, pl.ds(half, HALF)], wbuf, wsem)
    wcopy.start()
    lane = lax.broadcasted_iota(jnp.int32, (SUB, LANE), 1)
    gam = prm[1:2, 0:WIDTH]
    bet = prm[2:3, 0:WIDTH]

    def sub_step(k, s, carry):
        i = k * 4 + s
        slot = lax.rem(i, 2)

        @pl.when(i + 1 < ROWS // SUB)
        def _():
            load(i + 1, 1 - slot).start()

        load(i, slot).wait()
        row = pl.multiple_of(i * SUB, SUB)

        def means(g):
            for j in range(TG):
                v = fbuf[slot, g * TG + j].astype(F32)
                mb[g * TG + j] = jnp.broadcast_to(jnp.sum(v, axis=-1, keepdims=True) * (1.0 / WIDTH), (SUB, LANE))

        def scales(g):
            for j in range(TG):
                t = g * TG + j
                cv = fbuf[slot, t].astype(F32) - rep(mb[t])
                var = jnp.sum(cv * cv, axis=-1, keepdims=True) * (1.0 / WIDTH)
                ib[t] = jnp.broadcast_to(lax.rsqrt(var + LN_EPS), (SUB, LANE))

        def sums(g):
            st = jnp.zeros((SUB, LANE), F32)
            part = jnp.zeros((SUB, WIDTH), F32)
            for j in range(TG):
                t = g * TG + j
                m = mb[t]
                inv = ib[t]
                part = part + (fbuf[slot, t].astype(F32) - rep(m)) * rep(inv)
                st = jnp.where(lane == j, m, jnp.where(lane == SIDE + j, inv, st))
            stat_ref[g, pl.ds(row, SUB), :] = st
            ab[...] += part

        ab[...] = jnp.zeros_like(ab)
        means(0)
        means(1)
        scales(0)

        def body(g, cr_):
            sums(g - 1)
            scales(g)
            means(g + 1)
            return cr_

        lax.fori_loop(1, 6, body, 0)
        sums(5)
        scales(6)
        sums(6)
        xh = ab[...] * (1.0 / TOKENS)
        xhm_ref[pl.ds(row, SUB), :] = xh
        prow[pl.ds(pl.multiple_of(s * SUB, SUB), SUB), :] = (xh * gam + bet).astype(BF16).astype(F32)
        return carry

    sends = []

    def relay(chunk, ss, rs, dev):
        cp = rcopy(pall.at[chunk], chunk, ss, rs, dev)
        cp.start()
        sends.append(cp)

    def pass_on(k):
        cx = dpx * 4 + k
        cy = dpy * 4 + k
        rcopy(pall.at[cx], cx, sx.at[k], rx.at[k], dpx).wait_recv()
        if k % 2 == 0:
            relay(cx, sy.at[4 + k // 2], ry.at[4 + k // 2], dpy)
        relay(cx, sc.at[4 + k], rc.at[4 + k], dpc)
        rcopy(pall.at[cy], cy, sy.at[k], ry.at[k], dpy).wait_recv()
        if k % 2 == 1:
            relay(cy, sx.at[4 + k // 2], rx.at[4 + k // 2], dpx)
        relay(cy, sc.at[8 + k], rc.at[8 + k], dpc)

    locals_ = []
    for k in range(4):
        lax.fori_loop(0, 4, functools.partial(sub_step, k), 0)
        psend[k, 0:WIDTH, :] = prow[...].T
        psend[k, WIDTH:PROWS, :] = jnp.broadcast_to(prm[3:4, k * 128:(k + 1) * 128], (8, 128))
        if k == 0:
            pl.semaphore_wait(bar, 3 + PEERS)
        ch = dp * 4 + k
        for cp in (rcopy(psend.at[k], ch, sx.at[k], rx.at[k], dpx),
                   rcopy(psend.at[k], ch, sy.at[k], ry.at[k], dpy),
                   rcopy(psend.at[k], ch, sc.at[k], rc.at[k], dpc)):
            cp.start()
            sends.append(cp)
        lc = pltpu.make_async_copy(psend.at[k], pall.at[ch], loc.at[k])
        lc.start()
        locals_.append(lc)
        if k >= 2:
            pass_on(k - 2)

    wcopy.wait()

    def turn(n, cr_):
        cols = pl.ds(pl.multiple_of(n * LANE, LANE), 128)
        wt_ref[cols, :] = wbuf[:, cols].T
        bv = prm[0:1, pl.ds(pl.multiple_of(half + n * LANE, LANE), LANE)]
        bb_ref[cols, :] = jnp.broadcast_to(bv, (LANE, LANE)).T
        return cr_

    lax.fori_loop(0, HALF // LANE, turn, 0)

    def out(src, dst, i):
        cp = pltpu.make_async_copy(src, dst, osem.at[i])
        cp.start()
        locals_.append(cp)

    for cp in locals_:
        cp.wait()
    locals_.clear()
    out(wt_ref, wt_o, 0)
    out(bb_ref, bb_o, 1)
    for k in range(4):
        ch = dpc * 4 + k
        rcopy(pall.at[ch], ch, sc.at[k], rc.at[k], dpc).wait_recv()
    pass_on(2)

    ploads, fwd_block, dl_block = block_code(0, pall, wt_ref, bb_ref, loss_ref, dlt, ering, ptb, pbuf, ylab, sbuf, db_ref,
                                             iota_ref, psem, ss, rs)
    iota_ref[...] = lax.broadcasted_iota(jnp.int32, (LT, LANE), 0).astype(F32)
    db_ref[...] = jnp.zeros_like(db_ref)
    loss_ref[...] = jnp.zeros_like(loss_ref)
    for cp in ploads(0):
        cp.start()

    def own_fwd(r, cr_):
        fwd_block(r, OWN)
        return cr_

    def own_dl(r, cr_):
        dl_block(r)
        return cr_

    def dpool_block(i, cr_):
        lanes = pl.ds(pl.multiple_of(i * RB, RB), RB)
        dpa[i] = jnp.dot(wbuf[...], dlt[:, lanes], preferred_element_type=F32)
        return cr_

    lax.fori_loop(0, OWN, own_fwd, 0)
    out(ptb, ptb_o, 2)
    pass_on(3)
    lax.fori_loop(0, OWN, own_dl, 0)
    out(dlt, dlt_o, 3)
    out(db_ref, db_o, 4)
    lax.fori_loop(0, OWN, dpool_block, 0)
    d2c = pltpu.make_async_remote_copy(src_ref=dpa.at[pl.ds((1 - c) * 2, 2)], dst_ref=d2d, send_sem=cs, recv_sem=cr,
                                       device_id={"dp": dpc}, device_id_type=MESH)
    d2c.start()
    d2c.wait()
    for h in range(2):
        d2d[h] = d2d[h] + dpa[c * 2 + h]
    out(d2d, own_o, 5)
    for k in range(4):
        cd = dpd * 4 + k
        if k % 2 == 0:
            rcopy(pall.at[cd], cd, sy.at[4 + k // 2], ry.at[4 + k // 2], dpy).wait_recv()
        else:
            rcopy(pall.at[cd], cd, sx.at[4 + k // 2], rx.at[4 + k // 2], dpx).wait_recv()
        relay(cd, sc.at[12 + k], rc.at[12 + k], dpc)
    for q, d in enumerate((dpx, dpy, dpd)):
        for k in range(4):
            ch = (d + 1 - 2 * c) * 4 + k
            i = q * 4 + 4 + k
            rcopy(pall.at[ch], ch, sc.at[i], rc.at[i], dpc).wait_recv()
    for cp in sends:
        cp.wait_send()
    for cp in locals_:
        cp.wait()


dma = pltpu.SemaphoreType.DMA
V = pltpu.VMEM
OWNR = OWN * RB


def spec(space):
    return pl.BlockSpec(memory_space=space)


def shape(*dims, dtype=F32):
    return jax.ShapeDtypeStruct(dims, dtype)


def block_scratch(n, lanes):
    return [V((HALF, lanes), BF16), V((OWN, HALF, RB), F32), V((WIDTH, lanes), BF16), V((2, 2, PROWS, LANE), F32),
            V((n, 8, RB), F32), V((n, PEERS + 1, 4, RB), F32), V((HALF, LANE), F32), V((LT, LANE), F32)]


def ln_gather(f_t, prm, w):
    return pl.pallas_call(
        ln_gather_kernel,
        out_shape=(shape(BATCH // LANE, PROWS, LANE), shape(ROWS, WIDTH), shape(7, ROWS, LANE), shape(1, RB),
                   shape(HALF, WIDTH, dtype=BF16), shape(HALF, LANE), shape(HALF, OWNR, dtype=BF16),
                   shape(WIDTH, OWNR, dtype=BF16), shape(HALF, LANE), shape(2, WIDTH, RB)),
        in_specs=[spec(pl.ANY), spec(V), spec(pl.ANY)],
        out_specs=(spec(pl.ANY),) + (spec(V),) * 3 + (spec(pl.ANY),) * 6,
        scratch_shapes=[V((2, TOKENS, SUB, WIDTH), BF16), V((LANE, WIDTH), F32), V((4, PROWS, LANE), F32),
                        V((WIDTH, HALF), BF16), V((TOKENS, SUB, LANE), F32), V((TOKENS, SUB, LANE), F32), V((SUB, WIDTH), F32),
                        V((HALF, WIDTH), BF16), V((HALF, LANE), F32)] + block_scratch(OWN, OWNR) +
                       [V((OWN, WIDTH, RB), F32), V((2, WIDTH, RB), F32),
                        dma((2,)), dma, dma((4,)), dma((6,)), dma((6,)), dma((16,)), dma((6,)), dma((6,)), dma((16,)),
                        dma((2, 2)), dma((OWN, PEERS)), dma((OWN, PEERS)), dma, dma, dma((6,))],
        compiler_params=pltpu.CompilerParams(collective_id=0, has_side_effects=True, vmem_limit_bytes=VMEM_ALL),
        name="ln_gather",
    )(f_t, prm, w)


def head_kernel(pall, wt_h, b_h, xhm_ref, dlt_h, ptb_h, db_h, own_h, loss0, dpool_ref, dwo, dwr, dbo, loss_ref, grad_ref,
                dlt, ering, ptb, pbuf, ylab, sbuf, db_ref, iota_ref, wt_ref, b_ref, d2d, dpa, ubuf, dbuf, dwt, gbuf,
                psem, ss, rs, us, ur, ds_, dr, dls, dss, dsr, bs, br, gs, gr, xsem, osem, lsem):
    z, dp, y, x, c = coords()
    dpc = dp + 1 - 2 * c

    bar = pltpu.get_barrier_semaphore()
    for j in range(PEERS):
        pl.semaphore_signal(bar, inc=1, device_id=peer(j), device_id_type=MESH)
        pl.semaphore_signal(bar, inc=1, device_id={"dp": lax.rem(dp + 1 + j, 8)}, device_id_type=MESH)

    ploads, fwd_block, dl_block = block_code(OWN, pall, wt_ref, b_ref, loss_ref, dlt, ering, ptb, pbuf, ylab, sbuf, db_ref,
                                             iota_ref, psem, ss, rs)
    own_lanes = slice(0, OWNR)
    loads = [pltpu.make_async_copy(src, dst, lsem.at[i]) for i, (src, dst) in enumerate((
        (own_h, d2d), (wt_h, wt_ref), (b_h, b_ref), (db_h, db_ref), (ptb_h, ptb.at[:, own_lanes]), (dlt_h, dlt.at[:, own_lanes])))]
    for cp in loads[0:2]:
        cp.start()
    for cp in ploads(OWN):
        cp.start()
    for cp in loads[2:]:
        cp.start()
    half = pl.multiple_of(c * HALF, LANE)
    iota_ref[...] = lax.broadcasted_iota(jnp.int32, (LT, LANE), 0).astype(F32)
    loss_ref[...] = loss0[...]
    loads[0].wait()
    pl.semaphore_wait(bar, 2 * PEERS)

    def part(j):
        return pl.ds(pl.multiple_of(j * ARW, ARW), ARW)

    def up(j):
        return pltpu.make_async_remote_copy(src_ref=ubuf.at[:, part(j), :], dst_ref=ubuf.at[:, part(j), :],
                                            send_sem=us.at[j], recv_sem=ur.at[j],
                                            device_id={"tp": jnp.minimum(z + 1, 3)}, device_id_type=MESH)

    def down(j):
        return pltpu.make_async_remote_copy(src_ref=dpa.at[:, part(j), :], dst_ref=dbuf.at[:, part(j), :],
                                            send_sem=ds_.at[j], recv_sem=dr.at[j],
                                            device_id={"tp": jnp.maximum(z - 1, 0)}, device_id_type=MESH)

    @pl.when(z == 0)
    def _():
        for j in range(ARC):
            ubuf[:, part(j), :] = d2d[:, part(j), :]
            up(j).start()

    @pl.when(z == 3)
    def _():
        for j in range(ARC):
            dpa[:, part(j), :] = d2d[:, part(j), :]
            down(j).start()

    def tick(t):
        j = t - 2 * z

        @pl.when((z >= 1) & (j >= 0) & (j < ARC))
        def _():
            up(j).wait_recv()
            ubuf[:, part(j), :] += d2d[:, part(j), :]

            @pl.when(z < 3)
            def _():
                up(j).start()

        k = t - 2 * (3 - z)

        @pl.when((z <= 2) & (k >= 0) & (k < ARC))
        def _():
            down(k).wait_recv()

            @pl.when(z > 0)
            def _():
                dpa[:, part(k), :] = dbuf[:, part(k), :] + d2d[:, part(k), :]
                down(k).start()

    for cp in loads[1:4]:
        cp.wait()

    def rest(r, cr_):
        fwd_block(r, NB)

        @pl.when(r >= OWN + 2)
        def _():
            dl_block(r - 2)

        tick(r - OWN)
        return cr_

    def last_dl(r, cr_):
        dl_block(r)
        return cr_

    lax.fori_loop(OWN, NB, rest, 0)
    lax.fori_loop(NB - 2, NB, last_dl, 0)
    for cp in loads[4:]:
        cp.wait()

    for n in range(NT):
        row = jnp.sum(db_ref[n * TILE:(n + 1) * TILE, :].T, axis=0, keepdims=True)
        dbo[0:1, pl.ds(pl.multiple_of(half + n * TILE, 128), TILE)] = row
    dbc = pltpu.make_async_remote_copy(src_ref=dbo.at[:, pl.ds(half, HALF)], dst_ref=dbo.at[:, pl.ds(half, HALF)], send_sem=bs, recv_sem=br,
                                       device_id={"dp": dpc}, device_id_type=MESH)
    dbc.start()

    xcopies = [pltpu.make_async_copy(xhm_ref.at[:, q * RB:(q + 1) * RB], ering.at[0, q * ROWS:(q + 1) * ROWS, :], xsem.at[q])
               for q in range(3)]
    for cp in xcopies:
        cp.start()

    def dw_local(n):
        slot = lax.rem(n, 2)
        return pltpu.make_async_copy(dwt.at[slot], dwo.at[:, pl.ds(pl.multiple_of(n * TILE, TILE), TILE)], dls.at[slot])

    def dw_remote(n):
        slot = lax.rem(n, 2)
        return pltpu.make_async_remote_copy(
            src_ref=dwt.at[slot], dst_ref=dwr.at[:, pl.ds(pl.multiple_of(n * TILE, TILE), TILE)],
            send_sem=dss.at[slot], recv_sem=dsr.at[n], device_id={"dp": dpc}, device_id_type=MESH)

    def dw_step(n, cr_):
        @pl.when(n >= 2)
        def _():
            dw_local(n - 2).wait()
            dw_remote(n - 2).wait_send()

        rows = pl.ds(pl.multiple_of(n * TILE, TILE), TILE)
        dwt[lax.rem(n, 2)] = lax.dot_general(ptb[...], dlt[rows, :], (((1,), (1,)), ((), ())), preferred_element_type=F32)
        dw_local(n).start()
        dw_remote(n).start()
        tick(n + NB - OWN)
        return cr_

    lax.fori_loop(0, NT, dw_step, 0)

    for cp in xcopies:
        cp.wait()
    for j in range(WIDTH // LANE):
        rows = slice(j * LANE, (j + 1) * LANE)
        tot = jnp.where(z < 3, dbuf[:, rows, :], 0.0) + ubuf[:, rows, :]
        tt = jnp.concatenate([tot[0], tot[1]], axis=1).T
        q, lo = j // 2, (j % 2) * 128
        ering[1, q * ROWS:(q + 1) * ROWS, lo:lo + 128] = tt
        cols = slice(j * 128, (j + 1) * 128)
        gbuf[7, 0:1, cols] = jnp.sum(tt * ering[0, q * ROWS:(q + 1) * ROWS, lo:lo + 128], axis=0, keepdims=True)
        gbuf[7, 1:2, cols] = jnp.sum(tt, axis=0, keepdims=True)
    ocopies = [pltpu.make_async_copy(ering.at[1, q * ROWS:(q + 1) * ROWS, :], dpool_ref.at[:, q * RB:(q + 1) * RB], osem.at[q])
               for q in range(3)]
    for cp in ocopies:
        cp.start()

    def gcopy(j, slot):
        return pltpu.make_async_remote_copy(src_ref=gbuf.at[7], dst_ref=gbuf.at[slot], send_sem=gs.at[j], recv_sem=gr.at[slot],
                                            device_id={"dp": lax.rem(dp + 1 + j, 8)}, device_id_type=MESH)

    for j in range(PEERS):
        gcopy(j, 6 - j).start()

    for n in (NT - 2, NT - 1):
        dw_local(n).wait()
        dw_remote(n).wait_send()

    def dw_recv(n, cr_):
        dw_remote(n).wait_recv()
        return cr_

    lax.fori_loop(0, NT, dw_recv, 0)
    dbc.wait_send()
    other = pl.ds(pl.multiple_of((1 - c) * HALF, 128), HALF)
    pltpu.make_async_remote_copy(src_ref=dbo.at[:, other], dst_ref=dbo.at[:, other], send_sem=bs, recv_sem=br,
                                 device_id={"dp": dpc}, device_id_type=MESH).wait_recv()
    for j in range(PEERS):
        gcopy(j, j).wait_recv()
        gcopy(j, j).wait_send()
    for cp in ocopies:
        cp.wait()
    grads = gbuf[7]
    for j in range(PEERS):
        grads = grads + gbuf[j]
    grad_ref[...] = grads

    @pl.when(z < 3)
    def _():
        for j in range(ARC):
            up(j).wait_send()

    @pl.when(z > 0)
    def _():
        for j in range(ARC):
            down(j).wait_send()


def head(pall, wt, bb, xhm, dlt, ptb, db, own, loss):
    return pl.pallas_call(
        head_kernel,
        out_shape=(shape(ROWS, WIDTH), shape(WIDTH, HALF), shape(WIDTH, HALF), shape(1, CLS), shape(1, RB), shape(2, WIDTH)),
        in_specs=[spec(pl.ANY)] * 8 + [spec(V)],
        out_specs=(spec(pl.ANY),) * 3 + (spec(V),) * 3,
        scratch_shapes=block_scratch(NB - OWN, BATCH) +
                       [V((HALF, WIDTH), BF16), V((HALF, LANE), F32)] + [V((2, WIDTH, RB), F32)] * 4 +
                       [V((2, WIDTH, TILE), F32), V((PEERS + 1, 2, WIDTH), F32),
                        dma((2, 2)), dma((NB - OWN, PEERS)), dma((NB - OWN, PEERS)),
                        dma((ARC,)), dma((ARC,)), dma((ARC,)), dma((ARC,)),
                        dma((2,)), dma((2,)), dma((NT,)), dma, dma, dma((PEERS,)), dma((PEERS,)), dma((3,)), dma((3,)), dma((6,))],
        compiler_params=pltpu.CompilerParams(collective_id=1, has_side_effects=True, vmem_limit_bytes=VMEM_ALL),
        name="head",
    )(pall, wt, bb, xhm, dlt, ptb, db, own, loss)


DROWS = WIDTH // (ROWS // SUB)


def ln_bwd_kernel(f_ref, stat_ref, dp_ref, prm, dwo, dwr, o_ref, dw_ref, mb, ib, kb, ub, cbuf, ls, ws):
    c = lax.rem(lax.axis_index("dp"), 2)
    i = pl.program_id(0)
    last = ROWS // SUB - 1

    def pull(i):
        slot = lax.rem(i, 2)
        rows = pl.ds(pl.multiple_of(i * DROWS, 8), DROWS)
        return [pltpu.make_async_copy(h.at[rows, :], cbuf.at[slot, q], ls.at[slot, q]) for q, h in enumerate((dwo, dwr))]

    def push(i):
        slot = lax.rem(i, 2)
        rows = pl.ds(pl.multiple_of(i * DROWS, 8), DROWS)
        return [pltpu.make_async_copy(cbuf.at[slot, q], dw_ref.at[rows, pl.ds(pl.multiple_of((c + q - 2 * c * q) * HALF, 128), HALF)],
                                      ws.at[slot, q]) for q in range(2)]

    @pl.when(i >= 2)
    def _():
        for cp in push(i - 2):
            cp.wait()

    for cp in pull(i):
        cp.start()

    @pl.when(i >= 1)
    def _():
        for cp in pull(i - 1):
            cp.wait()
        for cp in push(i - 1):
            cp.start()

    u = dp_ref[...] * prm[1:2, :] * (1.0 / TOKENS)
    ub[...] = u - jnp.sum(u, axis=-1, keepdims=True) * (1.0 / WIDTH)

    def spread(g):
        st = stat_ref[g]
        for j in range(TG):
            mb[g * TG + j] = jnp.broadcast_to(st[:, j:j + 1], (SUB, LANE))
            ib[g * TG + j] = jnp.broadcast_to(st[:, SIDE + j:SIDE + j + 1], (SUB, LANE))

    def project(g):
        for j in range(TG):
            t = g * TG + j
            d = f_ref[t].astype(F32) - rep(mb[t])
            inv = ib[t]
            kb[t] = (inv * inv * inv) * (jnp.sum(d * ub[...], axis=-1, keepdims=True) * (1.0 / WIDTH))

    def write(g):
        for j in range(TG):
            t = g * TG + j
            d = f_ref[t].astype(F32) - rep(mb[t])
            o_ref[t] = (rep(ib[t]) * ub[...] - rep(kb[t]) * d).astype(BF16)

    spread(0)
    spread(1)
    project(0)

    def body(g, cr_):
        write(g - 1)
        project(g)
        spread(g + 1)
        return cr_

    lax.fori_loop(1, 6, body, 0)
    write(5)
    project(6)
    write(6)

    @pl.when(i == last)
    def _():
        for cp in pull(i):
            cp.wait()
        for cp in push(i):
            cp.start()
        for cp in push(i - 1):
            cp.wait()
        for cp in push(i):
            cp.wait()


def ln_bwd(f_t, stat, dpool, prm, dwo, dwr):
    blk = pl.BlockSpec((TOKENS, SUB, WIDTH), lambda i: (0, i, 0))
    hbm = spec(pl.ANY)
    return pl.pallas_call(
        ln_bwd_kernel,
        grid=(ROWS // SUB,),
        out_shape=(jax.ShapeDtypeStruct((TOKENS, ROWS, WIDTH), BF16), jax.ShapeDtypeStruct((WIDTH, CLS), F32)),
        in_specs=[blk, pl.BlockSpec((7, SUB, 128), lambda i: (0, i, 0)),
                  pl.BlockSpec((SUB, WIDTH), lambda i: (i, 0)), pl.BlockSpec((8, WIDTH), lambda i: (0, 0)), hbm, hbm],
        out_specs=(blk, hbm),
        scratch_shapes=[V((TOKENS, SUB, 128), F32), V((TOKENS, SUB, 128), F32), V((TOKENS, SUB, 128), F32), V((SUB, WIDTH), F32),
                        V((2, 2, DROWS, HALF), F32), pltpu.SemaphoreType.DMA((2, 2)), pltpu.SemaphoreType.DMA((2, 2))],
        name="ln_bwd",
    )(f_t, stat, dpool, prm, dwo, dwr)


def solution(mesh):
    def local(feats, gamma, beta, w, b, labels):
        f_t = jnp.transpose(feats, (1, 0, 2))

        def row(v):
            return jnp.pad(v.astype(F32), (0, CLS - v.shape[0]))

        zero = jnp.zeros((CLS,), F32)
        prm = jnp.stack([b, row(gamma), row(beta), row(labels), zero, zero, zero, zero])
        pall, xhm, stat, loss, wt, bb, dlt, ptb, db, own = ln_gather(f_t, prm, w)
        dpool, dwo, dwr, db, loss, grads = head(pall, wt, bb, xhm, dlt, ptb, db, own, loss)
        df_t, dw = ln_bwd(f_t, stat, dpool, prm, dwo, dwr)
        return jnp.sum(loss) / BATCH, jnp.transpose(df_t, (1, 0, 2)), dw, db[0], grads[0], grads[1]

    return jax.shard_map(local, mesh=mesh, in_specs=(P("dp", None, None), P(), P(), P(None, "tp"), P("tp"), P("dp")),
                         out_specs=(P(), P("dp", None, None), P(None, "tp"), P("tp"), P(), P()), check_vma=False)
```

```python
import functools
import jax
import jax.numpy as jnp
from jax import lax
from jax.experimental import pallas as pl
from jax.experimental.pallas import tpu as pltpu
from jax.sharding import PartitionSpec as P

VALID_CLASSES = 21841
LN_EPS = 1e-5
SMOOTH = 0.1
BATCH = 4096
TOKENS = 49
WIDTH = 768
HALF = 2816
TILE = 256
NT = HALF // TILE
LT = 1408
ET = 704
CLS = 2 * HALF
RB = 256
NB = BATCH // RB
ROWS = 512
SUB = 32
PROWS = WIDTH + 8
ARW = 64
ARC = WIDTH // ARW
LANE = 128
LAG = 3
TG = 7
SIDE = 64
PEERS = 7
VMEM_ALL = 64 * 1024 * 1024 - 65536
F32 = jnp.float32
BF16 = jnp.bfloat16


def coords():
    z = lax.axis_index("tp")
    dp = lax.axis_index("dp")
    c = lax.rem(dp, 2)
    x = lax.rem(dp // 2, 2)
    y = dp // 4
    return z, dp, y, x, c


OWN = 4
MESH = pl.DeviceIdType.MESH
C0 = (SMOOTH / VALID_CLASSES) / BATCH
C1 = C0 + (1.0 - SMOOTH) / BATCH


def peer(j):
    z, dp, y, x, c = coords()
    p = lax.rem(z * 2 + c + 1 + j, PEERS + 1)
    return {"tp": p // 2, "dp": dp - c + lax.rem(p, 2)}


def block_code(first, pall, wt_ref, b_ref, loss_ref, dlt, ering, ptb, pbuf, ylab, sbuf, db_ref, iota_ref, psem, ss, rs):
    z, dp, y, x, c = coords()
    colbase = (z * 2 + c) * HALF
    colbase_f = colbase.astype(F32)
    limit_f = (VALID_CLASSES - colbase).astype(F32)
    halves = range(2)

    def chunk_of(r, h):
        q = r // 2
        qc = q // 2
        gx = lax.rem(x + lax.rem(qc, 2), 2)
        gy = lax.rem(y + qc // 2, 2)
        return (gy * 4 + gx * 2 + lax.rem(q, 2)) * 4 + lax.rem(r, 2) * 2 + h

    def ploads(r):
        slot = lax.rem(r, 2)
        return [pltpu.make_async_copy(pall.at[chunk_of(r, h)], pbuf.at[slot, h], psem.at[slot, h]) for h in halves]

    def shifted(yb, off, n):
        return jnp.broadcast_to((yb - off)[None], (n // 8, 8, RB)).reshape(n, RB)

    def ids(n):
        v = iota_ref[0:n, :]
        return jnp.concatenate([v, v], axis=1)

    def fold(v):
        return v.reshape(v.shape[0] // 8, 8, RB)

    def scopy(r, j, slot):
        i = r - first
        return pltpu.make_async_remote_copy(src_ref=sbuf.at[i, PEERS], dst_ref=sbuf.at[i, slot], send_sem=ss.at[i, j],
                                            recv_sem=rs.at[i, slot], device_id=peer(j), device_id_type=MESH)

    def fwd_block(r, stop, fused=0):
        slot = lax.rem(r, 2)
        if fused:
            dl_tile = dl_stats(r - LAG)

        @pl.when(r + 1 < stop)
        def _():
            for cp in ploads(r + 1):
                cp.start()

        for cp in ploads(r):
            cp.wait()
        lanes = pl.ds(pl.multiple_of(r * RB, RB), RB)
        ptb[:, lanes] = jnp.concatenate([pbuf[slot, h, 0:WIDTH, :] for h in halves], axis=1).astype(BF16)
        yb = jnp.concatenate([pbuf[slot, h, WIDTH:PROWS, :] for h in halves], axis=1) - colbase_f
        ylab[r - first] = yb
        es = lax.rem(r, OWN)
        zero = jnp.zeros((8, RB), F32)
        mx, tg, vs = jnp.full((8, RB), -3e38, F32), zero, zero
        for n in range(HALF // LT):
            full = jnp.dot(wt_ref[n * LT:(n + 1) * LT, :], ptb[:, lanes], preferred_element_type=F32)
            if fused:
                dl_tile(2 * n, 0)
                dl_tile(2 * n + 1, n)
            for lo, size, masked in (((0, LT, 0),) if n == 0 else ((0, ET, 0), (ET, ET, 1))):
                row = n * LT + lo
                bb = b_ref[row:row + size, :]
                l = full[lo:lo + size] + jnp.concatenate([bb, bb], axis=1)
                tg = tg + fold(jnp.where(ids(size) == shifted(yb, float(row), size), l, 0.0)).sum(axis=0)
                if masked:
                    ok = ids(size) < limit_f - float(row)
                    vs = vs + fold(jnp.where(ok, l, 0.0)).sum(axis=0)
                    l = jnp.where(ok, l, -1e30)
                else:
                    vs = vs + fold(l).sum(axis=0)
                ering[es, row:row + size, :] = l
                mx = jnp.maximum(mx, fold(l).max(axis=0))
        m = jnp.max(mx, axis=0, keepdims=True)
        mb = jnp.broadcast_to(m, (ET, RB))

        def pass2(n, s):
            rows = pl.ds(pl.multiple_of(n * ET, ET), ET)
            e = jnp.exp(ering[es, rows, :] - mb)
            ering[es, rows, :] = e
            return s + fold(e).sum(axis=0)

        s = lax.fori_loop(0, HALF // ET, pass2, zero)
        tops = [m] + [jnp.sum(v, axis=0, keepdims=True) for v in (s, tg, vs)]
        for q, v in enumerate(tops):
            sbuf[r - first, PEERS, q:q + 1, :] = v
        for j in range(PEERS):
            scopy(r, j, PEERS - 1 - j).start()

    def dl_stats(r):
        es = lax.rem(r, OWN)
        for j in range(PEERS):
            cp = scopy(r, j, j)
            cp.wait_recv()
            cp.wait_send()
        i = r - first
        mown = sbuf[i, PEERS, 0:1, :]
        gm = mown
        for j in range(PEERS):
            gm = jnp.maximum(gm, sbuf[i, j, 0:1, :])
        zs, ts, vs = (jnp.zeros_like(gm) for _ in range(3))
        for j in range(PEERS + 1):
            zs = zs + sbuf[i, j, 1:2, :] * jnp.exp(sbuf[i, j, 0:1, :] - gm)
            ts = ts + sbuf[i, j, 2:3, :]
            vs = vs + sbuf[i, j, 3:4, :]
        loss_ref[...] += gm + jnp.log(zs) - (1.0 - SMOOTH) * ts - (SMOOTH / VALID_CLASSES) * vs
        scb = jnp.broadcast_to(jnp.exp(mown - gm) / (zs * BATCH), (ET, RB))
        yb = ylab[i]
        lanes = pl.ds(pl.multiple_of(r * RB, RB), RB)

        def tile(n, masked):
            rows = slice(n * ET, n * ET + ET) if isinstance(n, int) else pl.ds(pl.multiple_of(n * ET, ET), ET)
            off = lax.convert_element_type(n * ET, F32)
            base = jnp.where(ids(ET) < limit_f - off, C0, 0.0) if masked else C0
            d = ering[es, rows, :] * scb - jnp.where(ids(ET) == shifted(yb, off, ET), C1, base)
            db_ref[rows, :] += d[:, 0:LANE] + d[:, LANE:RB]
            dlt[rows, lanes] = d.astype(BF16)

        return tile

    def dl_block(r):
        tile = dl_stats(r)

        def plain(n, cr_):
            tile(n, 0)
            return cr_

        lax.fori_loop(0, HALF // ET - 1, plain, 0)
        tile(HALF // ET - 1, 1)

    return ploads, fwd_block, dl_block


def rep(v):
    return jnp.concatenate([v] * (WIDTH // 128), axis=1)


def ln_gather_kernel(f_hbm, prm, w_hbm, pall, xhm_ref, stat_ref, loss_ref, wt_o, bb_o, dlt_o, ptb_o, db_o, own_o,
                     fbuf, prow, psend, wbuf, mb, ib, ab, wt_ref, bb_ref, dlt, ering, ptb, pbuf, ylab, sbuf, db_ref, iota_ref,
                     dpa, d2d, fsem, wsem, loc, sx, sy, sc, rx, ry, rc, psem, ss, rs, cs, cr, osem):
    z, dp, y, x, c = coords()
    dpx = dp + 2 - 4 * x
    dpy = dp + 4 - 8 * y
    dpc = dp + 1 - 2 * c
    dpd = dpx + 4 - 8 * y

    bar = pltpu.get_barrier_semaphore()
    for d in (dpx, dpy, dpc):
        pl.semaphore_signal(bar, inc=1, device_id={"dp": d}, device_id_type=MESH)
    for j in range(PEERS):
        pl.semaphore_signal(bar, inc=1, device_id=peer(j), device_id_type=MESH)

    def load(i, slot):
        return pltpu.make_async_copy(f_hbm.at[:, pl.ds(pl.multiple_of(i * SUB, SUB), SUB), :], fbuf.at[slot], fsem.at[slot])

    def rcopy(src, chunk, ss, rs, dev):
        return pltpu.make_async_remote_copy(src_ref=src, dst_ref=pall.at[chunk], send_sem=ss, recv_sem=rs,
                                            device_id={"dp": dev}, device_id_type=pl.DeviceIdType.MESH)

    load(0, 0).start()
    half = pl.multiple_of(c * HALF, 128)
    wcopy = pltpu.make_async_copy(w_hbm.at[:, pl.ds(half, HALF)], wbuf, wsem)
    wcopy.start()
    lane = lax.broadcasted_iota(jnp.int32, (SUB, LANE), 1)
    gam = prm[1:2, 0:WIDTH]
    bet = prm[2:3, 0:WIDTH]

    def sub_step(k, s, carry):
        i = k * 4 + s
        slot = lax.rem(i, 2)

        @pl.when(i + 1 < ROWS // SUB)
        def _():
            load(i + 1, 1 - slot).start()

        load(i, slot).wait()
        row = pl.multiple_of(i * SUB, SUB)

        def means(g):
            for j in range(TG):
                v = fbuf[slot, g * TG + j].astype(F32)
                mb[g * TG + j] = jnp.broadcast_to(jnp.sum(v, axis=-1, keepdims=True) * (1.0 / WIDTH), (SUB, LANE))

        def scales(g):
            for j in range(TG):
                t = g * TG + j
                cv = fbuf[slot, t].astype(F32) - rep(mb[t])
                var = jnp.sum(cv * cv, axis=-1, keepdims=True) * (1.0 / WIDTH)
                ib[t] = jnp.broadcast_to(lax.rsqrt(var + LN_EPS), (SUB, LANE))

        def sums(g):
            st = jnp.zeros((SUB, LANE), F32)
            part = jnp.zeros((SUB, WIDTH), F32)
            for j in range(TG):
                t = g * TG + j
                m = mb[t]
                inv = ib[t]
                part = part + (fbuf[slot, t].astype(F32) - rep(m)) * rep(inv)
                st = jnp.where(lane == j, m, jnp.where(lane == SIDE + j, inv, st))
            stat_ref[g, pl.ds(row, SUB), :] = st
            ab[...] += part

        ab[...] = jnp.zeros_like(ab)
        means(0)
        means(1)
        scales(0)

        def body(g, cr_):
            sums(g - 1)
            scales(g)
            means(g + 1)
            return cr_

        lax.fori_loop(1, 6, body, 0)
        sums(5)
        scales(6)
        sums(6)
        xh = ab[...] * (1.0 / TOKENS)
        xhm_ref[pl.ds(row, SUB), :] = xh
        prow[pl.ds(pl.multiple_of(s * SUB, SUB), SUB), :] = (xh * gam + bet).astype(BF16).astype(F32)
        return carry

    sends = []

    def relay(chunk, ss, rs, dev):
        cp = rcopy(pall.at[chunk], chunk, ss, rs, dev)
        cp.start()
        sends.append(cp)

    def pass_on(k):
        cx = dpx * 4 + k
        cy = dpy * 4 + k
        rcopy(pall.at[cx], cx, sx.at[k], rx.at[k], dpx).wait_recv()
        if k % 2 == 0:
            relay(cx, sy.at[4 + k // 2], ry.at[4 + k // 2], dpy)
        relay(cx, sc.at[4 + k], rc.at[4 + k], dpc)
        rcopy(pall.at[cy], cy, sy.at[k], ry.at[k], dpy).wait_recv()
        if k % 2 == 1:
            relay(cy, sx.at[4 + k // 2], rx.at[4 + k // 2], dpx)
        relay(cy, sc.at[8 + k], rc.at[8 + k], dpc)

    locals_ = []
    for k in range(4):
        lax.fori_loop(0, 4, functools.partial(sub_step, k), 0)
        psend[k, 0:WIDTH, :] = prow[...].T
        psend[k, WIDTH:PROWS, :] = jnp.broadcast_to(prm[3:4, k * 128:(k + 1) * 128], (8, 128))
        if k == 0:
            pl.semaphore_wait(bar, 3 + PEERS)
        ch = dp * 4 + k
        for cp in (rcopy(psend.at[k], ch, sx.at[k], rx.at[k], dpx),
                   rcopy(psend.at[k], ch, sy.at[k], ry.at[k], dpy),
                   rcopy(psend.at[k], ch, sc.at[k], rc.at[k], dpc)):
            cp.start()
            sends.append(cp)
        lc = pltpu.make_async_copy(psend.at[k], pall.at[ch], loc.at[k])
        lc.start()
        locals_.append(lc)
        if k >= 2:
            pass_on(k - 2)

    wcopy.wait()

    def turn(n, cr_):
        cols = pl.ds(pl.multiple_of(n * LANE, LANE), 128)
        wt_ref[cols, :] = wbuf[:, cols].T
        bv = prm[0:1, pl.ds(pl.multiple_of(half + n * LANE, LANE), LANE)]
        bb_ref[cols, :] = jnp.broadcast_to(bv, (LANE, LANE)).T
        return cr_

    lax.fori_loop(0, HALF // LANE, turn, 0)

    def out(src, dst, i):
        cp = pltpu.make_async_copy(src, dst, osem.at[i])
        cp.start()
        locals_.append(cp)

    for cp in locals_:
        cp.wait()
    locals_.clear()
    out(wt_ref, wt_o, 0)
    out(bb_ref, bb_o, 1)
    for k in range(4):
        ch = dpc * 4 + k
        rcopy(pall.at[ch], ch, sc.at[k], rc.at[k], dpc).wait_recv()
    pass_on(2)

    ploads, fwd_block, dl_block = block_code(0, pall, wt_ref, bb_ref, loss_ref, dlt, ering, ptb, pbuf, ylab, sbuf, db_ref,
                                             iota_ref, psem, ss, rs)
    iota_ref[...] = lax.broadcasted_iota(jnp.int32, (LT, LANE), 0).astype(F32)
    db_ref[...] = jnp.zeros_like(db_ref)
    loss_ref[...] = jnp.zeros_like(loss_ref)
    for cp in ploads(0):
        cp.start()

    def own_fwd(r, cr_):
        fwd_block(r, OWN)
        return cr_

    def own_dl(r, cr_):
        dl_block(r)
        return cr_

    def dpool_block(i, cr_):
        lanes = pl.ds(pl.multiple_of(i * RB, RB), RB)
        dpa[i] = jnp.dot(wbuf[...], dlt[:, lanes], preferred_element_type=F32)
        return cr_

    lax.fori_loop(0, OWN, own_fwd, 0)
    out(ptb, ptb_o, 2)
    pass_on(3)
    lax.fori_loop(0, OWN, own_dl, 0)
    out(dlt, dlt_o, 3)
    out(db_ref, db_o, 4)
    lax.fori_loop(0, OWN, dpool_block, 0)
    d2c = pltpu.make_async_remote_copy(src_ref=dpa.at[pl.ds((1 - c) * 2, 2)], dst_ref=d2d, send_sem=cs, recv_sem=cr,
                                       device_id={"dp": dpc}, device_id_type=MESH)
    d2c.start()
    d2c.wait()
    for h in range(2):
        d2d[h] = d2d[h] + dpa[c * 2 + h]
    out(d2d, own_o, 5)
    for k in range(4):
        cd = dpd * 4 + k
        if k % 2 == 0:
            rcopy(pall.at[cd], cd, sy.at[4 + k // 2], ry.at[4 + k // 2], dpy).wait_recv()
        else:
            rcopy(pall.at[cd], cd, sx.at[4 + k // 2], rx.at[4 + k // 2], dpx).wait_recv()
        relay(cd, sc.at[12 + k], rc.at[12 + k], dpc)
    for q, d in enumerate((dpx, dpy, dpd)):
        for k in range(4):
            ch = (d + 1 - 2 * c) * 4 + k
            i = q * 4 + 4 + k
            rcopy(pall.at[ch], ch, sc.at[i], rc.at[i], dpc).wait_recv()
    for cp in sends:
        cp.wait_send()
    for cp in locals_:
        cp.wait()


dma = pltpu.SemaphoreType.DMA
V = pltpu.VMEM
OWNR = OWN * RB


def spec(space):
    return pl.BlockSpec(memory_space=space)


def shape(*dims, dtype=F32):
    return jax.ShapeDtypeStruct(dims, dtype)


def block_scratch(n, lanes):
    return [V((HALF, lanes), BF16), V((OWN, HALF, RB), F32), V((WIDTH, lanes), BF16), V((2, 2, PROWS, LANE), F32),
            V((n, 8, RB), F32), V((n, PEERS + 1, 4, RB), F32), V((HALF, LANE), F32), V((LT, LANE), F32)]


def ln_gather(f_t, prm, w):
    return pl.pallas_call(
        ln_gather_kernel,
        out_shape=(shape(BATCH // LANE, PROWS, LANE), shape(ROWS, WIDTH), shape(7, ROWS, LANE), shape(1, RB),
                   shape(HALF, WIDTH, dtype=BF16), shape(HALF, LANE), shape(HALF, OWNR, dtype=BF16),
                   shape(WIDTH, OWNR, dtype=BF16), shape(HALF, LANE), shape(2, WIDTH, RB)),
        in_specs=[spec(pl.ANY), spec(V), spec(pl.ANY)],
        out_specs=(spec(pl.ANY),) + (spec(V),) * 3 + (spec(pl.ANY),) * 6,
        scratch_shapes=[V((2, TOKENS, SUB, WIDTH), BF16), V((LANE, WIDTH), F32), V((4, PROWS, LANE), F32),
                        V((WIDTH, HALF), BF16), V((TOKENS, SUB, LANE), F32), V((TOKENS, SUB, LANE), F32), V((SUB, WIDTH), F32),
                        V((HALF, WIDTH), BF16), V((HALF, LANE), F32)] + block_scratch(OWN, OWNR) +
                       [V((OWN, WIDTH, RB), F32), V((2, WIDTH, RB), F32),
                        dma((2,)), dma, dma((4,)), dma((6,)), dma((6,)), dma((16,)), dma((6,)), dma((6,)), dma((16,)),
                        dma((2, 2)), dma((OWN, PEERS)), dma((OWN, PEERS)), dma, dma, dma((6,))],
        compiler_params=pltpu.CompilerParams(collective_id=0, has_side_effects=True, vmem_limit_bytes=VMEM_ALL),
        name="ln_gather",
    )(f_t, prm, w)


def head_kernel(pall, wt_h, b_h, xhm_ref, dlt_h, ptb_h, db_h, own_h, loss0, dpool_ref, dwo, dwr, dbo, loss_ref, grad_ref,
                dlt, ering, ptb, pbuf, ylab, sbuf, db_ref, iota_ref, wt_ref, b_ref, d2d, dpa, ubuf, dbuf, dwt, gbuf,
                psem, ss, rs, us, ur, ds_, dr, dls, dss, dsr, bs, br, gs, gr, xsem, osem, lsem):
    z, dp, y, x, c = coords()
    dpc = dp + 1 - 2 * c

    bar = pltpu.get_barrier_semaphore()
    for j in range(PEERS):
        pl.semaphore_signal(bar, inc=1, device_id=peer(j), device_id_type=MESH)
        pl.semaphore_signal(bar, inc=1, device_id={"dp": lax.rem(dp + 1 + j, 8)}, device_id_type=MESH)

    ploads, fwd_block, dl_block = block_code(OWN, pall, wt_ref, b_ref, loss_ref, dlt, ering, ptb, pbuf, ylab, sbuf, db_ref,
                                             iota_ref, psem, ss, rs)
    own_lanes = slice(0, OWNR)
    loads = [pltpu.make_async_copy(src, dst, lsem.at[i]) for i, (src, dst) in enumerate((
        (own_h, d2d), (wt_h, wt_ref), (b_h, b_ref), (db_h, db_ref), (ptb_h, ptb.at[:, own_lanes]), (dlt_h, dlt.at[:, own_lanes])))]
    for cp in loads[0:2]:
        cp.start()
    for cp in ploads(OWN):
        cp.start()
    for cp in loads[2:]:
        cp.start()
    half = pl.multiple_of(c * HALF, LANE)
    iota_ref[...] = lax.broadcasted_iota(jnp.int32, (LT, LANE), 0).astype(F32)
    loss_ref[...] = loss0[...]
    loads[0].wait()
    pl.semaphore_wait(bar, 2 * PEERS)

    def part(j):
        return pl.ds(pl.multiple_of(j * ARW, ARW), ARW)

    def up(j):
        return pltpu.make_async_remote_copy(src_ref=ubuf.at[:, part(j), :], dst_ref=ubuf.at[:, part(j), :],
                                            send_sem=us.at[j], recv_sem=ur.at[j],
                                            device_id={"tp": jnp.minimum(z + 1, 3)}, device_id_type=MESH)

    def down(j):
        return pltpu.make_async_remote_copy(src_ref=dpa.at[:, part(j), :], dst_ref=dbuf.at[:, part(j), :],
                                            send_sem=ds_.at[j], recv_sem=dr.at[j],
                                            device_id={"tp": jnp.maximum(z - 1, 0)}, device_id_type=MESH)

    def tick(t):
        j = t - 2 * z

        @pl.when((j >= 0) & (j < ARC))
        def _():
            @pl.when(z == 0)
            def _():
                ubuf[:, part(j), :] = d2d[:, part(j), :]

            @pl.when(z > 0)
            def _():
                up(j).wait_recv()
                ubuf[:, part(j), :] += d2d[:, part(j), :]

            @pl.when(z < 3)
            def _():
                up(j).start()

        k = t - 2 * (3 - z)

        @pl.when((k >= 0) & (k < ARC))
        def _():
            @pl.when(z == 3)
            def _():
                dpa[:, part(k), :] = d2d[:, part(k), :]

            @pl.when(z < 3)
            def _():
                down(k).wait_recv()

            @pl.when((z > 0) & (z < 3))
            def _():
                dpa[:, part(k), :] = dbuf[:, part(k), :] + d2d[:, part(k), :]

            @pl.when(z > 0)
            def _():
                down(k).start()

    for cp in loads[1:4]:
        cp.wait()

    def rest(fused, r, cr_):
        fwd_block(r, NB, fused)
        tick(r - OWN)
        return cr_

    def last_dl(r, cr_):
        dl_block(r)
        return cr_

    lax.fori_loop(OWN, OWN + LAG, functools.partial(rest, 0), 0)
    lax.fori_loop(OWN + LAG, NB, functools.partial(rest, 1), 0)
    lax.fori_loop(NB - LAG, NB, last_dl, 0)
    for cp in loads[4:]:
        cp.wait()

    for n in range(NT):
        row = jnp.sum(db_ref[n * TILE:(n + 1) * TILE, :].T, axis=0, keepdims=True)
        dbo[0:1, pl.ds(pl.multiple_of(half + n * TILE, 128), TILE)] = row
    dbc = pltpu.make_async_remote_copy(src_ref=dbo.at[:, pl.ds(half, HALF)], dst_ref=dbo.at[:, pl.ds(half, HALF)], send_sem=bs, recv_sem=br,
                                       device_id={"dp": dpc}, device_id_type=MESH)
    dbc.start()

    xcopies = [pltpu.make_async_copy(xhm_ref.at[:, q * RB:(q + 1) * RB], ering.at[0, q * ROWS:(q + 1) * ROWS, :], xsem.at[q])
               for q in range(3)]
    for cp in xcopies:
        cp.start()

    def dw_local(n):
        slot = lax.rem(n, 2)
        return pltpu.make_async_copy(dwt.at[slot], dwo.at[:, pl.ds(pl.multiple_of(n * TILE, TILE), TILE)], dls.at[slot])

    def dw_remote(n):
        slot = lax.rem(n, 2)
        return pltpu.make_async_remote_copy(
            src_ref=dwt.at[slot], dst_ref=dwr.at[:, pl.ds(pl.multiple_of(n * TILE, TILE), TILE)],
            send_sem=dss.at[slot], recv_sem=dsr.at[n], device_id={"dp": dpc}, device_id_type=MESH)

    def dw_step(n, cr_):
        @pl.when(n >= 2)
        def _():
            dw_local(n - 2).wait()
            dw_remote(n - 2).wait_send()

        rows = pl.ds(pl.multiple_of(n * TILE, TILE), TILE)
        dwt[lax.rem(n, 2)] = lax.dot_general(ptb[...], dlt[rows, :], (((1,), (1,)), ((), ())), preferred_element_type=F32)
        dw_local(n).start()
        dw_remote(n).start()

        @pl.when(lax.rem(n, 2) == 1)
        def _():
            tick(NB - OWN + n // 2)

        return cr_

    lax.fori_loop(0, NT, dw_step, 0)
    tick(NB - OWN + NT // 2)

    for cp in xcopies:
        cp.wait()
    for j in range(WIDTH // LANE):
        rows = slice(j * LANE, (j + 1) * LANE)
        tot = jnp.where(z < 3, dbuf[:, rows, :], 0.0) + ubuf[:, rows, :]
        tt = jnp.concatenate([tot[0], tot[1]], axis=1).T
        q, lo = j // 2, (j % 2) * 128
        ering[1, q * ROWS:(q + 1) * ROWS, lo:lo + 128] = tt
        cols = slice(j * 128, (j + 1) * 128)
        gbuf[7, 0:1, cols] = jnp.sum(tt * ering[0, q * ROWS:(q + 1) * ROWS, lo:lo + 128], axis=0, keepdims=True)
        gbuf[7, 1:2, cols] = jnp.sum(tt, axis=0, keepdims=True)
    ocopies = [pltpu.make_async_copy(ering.at[1, q * ROWS:(q + 1) * ROWS, :], dpool_ref.at[:, q * RB:(q + 1) * RB], osem.at[q])
               for q in range(3)]
    for cp in ocopies:
        cp.start()

    def gcopy(j, slot):
        return pltpu.make_async_remote_copy(src_ref=gbuf.at[7], dst_ref=gbuf.at[slot], send_sem=gs.at[j], recv_sem=gr.at[slot],
                                            device_id={"dp": lax.rem(dp + 1 + j, 8)}, device_id_type=MESH)

    for j in range(PEERS):
        gcopy(j, 6 - j).start()

    for n in (NT - 2, NT - 1):
        dw_local(n).wait()
        dw_remote(n).wait_send()

    def dw_recv(n, cr_):
        dw_remote(n).wait_recv()
        return cr_

    lax.fori_loop(0, NT, dw_recv, 0)
    dbc.wait_send()
    other = pl.ds(pl.multiple_of((1 - c) * HALF, 128), HALF)
    pltpu.make_async_remote_copy(src_ref=dbo.at[:, other], dst_ref=dbo.at[:, other], send_sem=bs, recv_sem=br,
                                 device_id={"dp": dpc}, device_id_type=MESH).wait_recv()
    for j in range(PEERS):
        gcopy(j, j).wait_recv()
        gcopy(j, j).wait_send()
    for cp in ocopies:
        cp.wait()
    grads = gbuf[7]
    for j in range(PEERS):
        grads = grads + gbuf[j]
    grad_ref[...] = grads

    @pl.when(z < 3)
    def _():
        for j in range(ARC):
            up(j).wait_send()

    @pl.when(z > 0)
    def _():
        for j in range(ARC):
            down(j).wait_send()


def head(pall, wt, bb, xhm, dlt, ptb, db, own, loss):
    return pl.pallas_call(
        head_kernel,
        out_shape=(shape(ROWS, WIDTH), shape(WIDTH, HALF), shape(WIDTH, HALF), shape(1, CLS), shape(1, RB), shape(2, WIDTH)),
        in_specs=[spec(pl.ANY)] * 8 + [spec(V)],
        out_specs=(spec(pl.ANY),) * 3 + (spec(V),) * 3,
        scratch_shapes=block_scratch(NB - OWN, BATCH) +
                       [V((HALF, WIDTH), BF16), V((HALF, LANE), F32)] + [V((2, WIDTH, RB), F32)] * 4 +
                       [V((2, WIDTH, TILE), F32), V((PEERS + 1, 2, WIDTH), F32),
                        dma((2, 2)), dma((NB - OWN, PEERS)), dma((NB - OWN, PEERS)),
                        dma((ARC,)), dma((ARC,)), dma((ARC,)), dma((ARC,)),
                        dma((2,)), dma((2,)), dma((NT,)), dma, dma, dma((PEERS,)), dma((PEERS,)), dma((3,)), dma((3,)), dma((6,))],
        compiler_params=pltpu.CompilerParams(collective_id=1, has_side_effects=True, vmem_limit_bytes=VMEM_ALL),
        name="head",
    )(pall, wt, bb, xhm, dlt, ptb, db, own, loss)


DROWS = WIDTH // (ROWS // SUB)


def ln_bwd_kernel(f_ref, stat_ref, dp_ref, prm, dwo, dwr, o_ref, dw_ref, mb, ib, kb, ub, cbuf, ls, ws):
    c = lax.rem(lax.axis_index("dp"), 2)
    i = pl.program_id(0)
    last = ROWS // SUB - 1

    def pull(i):
        slot = lax.rem(i, 2)
        rows = pl.ds(pl.multiple_of(i * DROWS, 8), DROWS)
        return [pltpu.make_async_copy(h.at[rows, :], cbuf.at[slot, q], ls.at[slot, q]) for q, h in enumerate((dwo, dwr))]

    def push(i):
        slot = lax.rem(i, 2)
        rows = pl.ds(pl.multiple_of(i * DROWS, 8), DROWS)
        return [pltpu.make_async_copy(cbuf.at[slot, q], dw_ref.at[rows, pl.ds(pl.multiple_of((c + q - 2 * c * q) * HALF, 128), HALF)],
                                      ws.at[slot, q]) for q in range(2)]

    @pl.when(i >= 2)
    def _():
        for cp in push(i - 2):
            cp.wait()

    for cp in pull(i):
        cp.start()

    @pl.when(i >= 1)
    def _():
        for cp in pull(i - 1):
            cp.wait()
        for cp in push(i - 1):
            cp.start()

    u = dp_ref[...] * prm[1:2, :] * (1.0 / TOKENS)
    ub[...] = u - jnp.sum(u, axis=-1, keepdims=True) * (1.0 / WIDTH)

    def spread(g):
        st = stat_ref[g]
        for j in range(TG):
            mb[g * TG + j] = jnp.broadcast_to(st[:, j:j + 1], (SUB, LANE))
            ib[g * TG + j] = jnp.broadcast_to(st[:, SIDE + j:SIDE + j + 1], (SUB, LANE))

    def project(g):
        for j in range(TG):
            t = g * TG + j
            d = f_ref[t].astype(F32) - rep(mb[t])
            inv = ib[t]
            kb[t] = (inv * inv * inv) * (jnp.sum(d * ub[...], axis=-1, keepdims=True) * (1.0 / WIDTH))

    def write(g):
        for j in range(TG):
            t = g * TG + j
            d = f_ref[t].astype(F32) - rep(mb[t])
            o_ref[t] = (rep(ib[t]) * ub[...] - rep(kb[t]) * d).astype(BF16)

    spread(0)
    spread(1)
    project(0)

    def body(g, cr_):
        write(g - 1)
        project(g)
        spread(g + 1)
        return cr_

    lax.fori_loop(1, 6, body, 0)
    write(5)
    project(6)
    write(6)

    @pl.when(i == last)
    def _():
        for cp in pull(i):
            cp.wait()
        for cp in push(i):
            cp.start()
        for cp in push(i - 1):
            cp.wait()
        for cp in push(i):
            cp.wait()


def ln_bwd(f_t, stat, dpool, prm, dwo, dwr):
    blk = pl.BlockSpec((TOKENS, SUB, WIDTH), lambda i: (0, i, 0))
    hbm = spec(pl.ANY)
    return pl.pallas_call(
        ln_bwd_kernel,
        grid=(ROWS // SUB,),
        out_shape=(jax.ShapeDtypeStruct((TOKENS, ROWS, WIDTH), BF16), jax.ShapeDtypeStruct((WIDTH, CLS), F32)),
        in_specs=[blk, pl.BlockSpec((7, SUB, 128), lambda i: (0, i, 0)),
                  pl.BlockSpec((SUB, WIDTH), lambda i: (i, 0)), pl.BlockSpec((8, WIDTH), lambda i: (0, 0)), hbm, hbm],
        out_specs=(blk, hbm),
        scratch_shapes=[V((TOKENS, SUB, 128), F32), V((TOKENS, SUB, 128), F32), V((TOKENS, SUB, 128), F32), V((SUB, WIDTH), F32),
                        V((2, 2, DROWS, HALF), F32), pltpu.SemaphoreType.DMA((2, 2)), pltpu.SemaphoreType.DMA((2, 2))],
        name="ln_bwd",
    )(f_t, stat, dpool, prm, dwo, dwr)


def solution(mesh):
    def local(feats, gamma, beta, w, b, labels):
        f_t = jnp.transpose(feats, (1, 0, 2))

        def row(v):
            return jnp.pad(v.astype(F32), (0, CLS - v.shape[0]))

        zero = jnp.zeros((CLS,), F32)
        prm = jnp.stack([b, row(gamma), row(beta), row(labels), zero, zero, zero, zero])
        pall, xhm, stat, loss, wt, bb, dlt, ptb, db, own = ln_gather(f_t, prm, w)
        dpool, dwo, dwr, db, loss, grads = head(pall, wt, bb, xhm, dlt, ptb, db, own, loss)
        df_t, dw = ln_bwd(f_t, stat, dpool, prm, dwo, dwr)
        return jnp.sum(loss) / BATCH, jnp.transpose(df_t, (1, 0, 2)), dw, db[0], grads[0], grads[1]

    return jax.shard_map(local, mesh=mesh, in_specs=(P("dp", None, None), P(), P(), P(None, "tp"), P("tp"), P("dp")),
                         out_specs=(P(), P("dp", None, None), P(None, "tp"), P("tp"), P(), P()), check_vma=False)
```
